128 devices in a mesh: branch: 4 (over z), vocab: 32 (over x, y, core).
Axes of the slice: x: 4, y: 4, z: 4, core: 2. Of those that a mesh axis runs over, the one named last changes fastest.
Arguments:
- teacher_hidden: bfloat16 [4, 768, 4096], P('branch', None, 'vocab'), may hold values from -300 to 300
- teacher_weight: bfloat16 [4, 4096, 32000], P('branch', None, 'vocab'), may hold values from -0.375 to 0.375
- student_hidden: bfloat16 [768, 4096], P('branch', 'vocab'), may hold values from -300 to 300
- student_weight: bfloat16 [4096, 32000], P(None, 'vocab'), may hold values from -0.375 to 0.375
- branch_weight: float32 [4], replicated, may hold values from 0.2 to 5
- assignment: int32 [4], replicated, may hold values from 0 to 3, each once
- targets: int32 [768], P('branch'), may hold values from 0 to 31999
Outputs:
- divergence: float32 [768], P('branch')
- target_loss: float32 [768], P('branch')
The draws below stay inside these ranges and needn't reach their ends.
Inputs may be any that keep to these rules, and one draw needn't show every extreme that they name: `assignment`: each branch number appears once.
All inputs are finite; a program needn't handle non-finite values.
Results may differ from the reference program's by a relative error of at most 0.0003.
Values may be sent and summed in bfloat16 or wider, within the bound.
No kernel may reach another device: no remote copies, remote signals or barrier semaphores. Data moves between devices by JAX's collectives and lax.ppermute only.
A program may use at most 128 MiB of HBM per device.

```python
import math
import jax
import jax.numpy as jnp

D = 4096
V = 32000
BRANCHES = 4
TOKENS = 768


def hidden_states(key, shape, plain_low, plain_high):
    first, second = jax.random.split(key)
    values = jax.random.normal(first, shape, jnp.float32)
    scales = jnp.exp(jax.random.uniform(second, shape[:-1] + (1,), jnp.float32, jnp.log(plain_low), jnp.log(plain_high)))
    values = values * scales
    return jnp.clip(values, -300.0, 300.0)


def draw_teacher_hidden(key, part):
    return hidden_states(jax.random.fold_in(key, 11), (BRANCHES, TOKENS, D), 0.4, 1.2).astype(jnp.bfloat16)


def draw_student_hidden(key, part):
    return hidden_states(jax.random.fold_in(key, 23), (TOKENS, D), 1.0, 1.0).astype(jnp.bfloat16)


def plant(entries, rng, smallest, high):
    extent = entries.shape
    spot = [jax.random.randint(jax.random.fold_in(rng, axis), (), 0, extent[axis]) for axis in range(len(extent))]
    entries = entries.at[tuple(spot)].set(smallest)
    longest = extent.index(max(extent))
    spot[longest] = (spot[longest] + 1) % extent[longest]
    return entries.at[tuple(spot)].set(high)


def block_levels(own_key, dims, shards, smallest, high):
    loudness = 1.0
    for dim, shards_of in shards:
        heights = jax.random.uniform(jax.random.fold_in(jax.random.fold_in(own_key, 6), dim), (shards_of,), jnp.float32, smallest / len(shards), high / len(shards))
        loudness = loudness * jnp.repeat(jnp.exp(heights), dims[dim] // shards_of).reshape((-1,) + (1,) * (len(dims) - 1 - dim))
    return loudness


def gaussian(key, extent, scale, limit, cuts=(), held_as=jnp.bfloat16):
    drawn = scale * jax.random.normal(key, extent, jnp.float32)
    if cuts:
        drawn = drawn * block_levels(key, extent, cuts, -0.22, 0.18)
    return jnp.clip(drawn, -limit, limit).astype(held_as)


def setup_inputs(seed: int = 0) -> dict:
    splits = jax.random.split(jax.random.key(seed), 8)
    return {
        "teacher_hidden": draw_teacher_hidden(jax.random.fold_in(splits[7], 71), 0),
        "teacher_weight": gaussian(splits[1], (BRANCHES, D, V), (D // 16) ** -0.5, 0.375, ((0, 4), (2, 32))),
        "student_hidden": draw_student_hidden(jax.random.fold_in(splits[7], 71), 0),
        "student_weight": gaussian(splits[3], (D, V), (D // 16) ** -0.5, 0.375, ((1, 32),)),
        "branch_weight": jnp.clip(jnp.exp(jax.random.uniform(splits[4], (BRANCHES,), jnp.float32, math.log(0.2), math.log(5.0))), 0.2, 5.0),
        "assignment": jax.random.permutation(splits[5], BRANCHES).astype(jnp.int32),
        "targets": plant(jax.random.randint(splits[6], (TOKENS,), 0, V), jax.random.fold_in(splits[6], 1), 0, V - 1).astype(jnp.int32),
    }


def log_total(logits):
    highest = jnp.max(logits, axis=-1, keepdims=True)
    return highest[..., 0] + jnp.log(jnp.sum(jnp.exp(logits - highest), axis=-1))


def reference(teacher_hidden, teacher_weight, student_hidden, student_weight, branch_weight, assignment, targets):
    share = branch_weight / jnp.sum(branch_weight)
    log_share = jnp.log(share)[assignment]
    stacked = []
    for group in range(BRANCHES):
        logits = jnp.dot(teacher_hidden[group], teacher_weight[group], preferred_element_type=jnp.float32)
        stacked.append(logits - log_total(logits)[:, None] + log_share[group])
    stacked = jnp.stack(stacked, axis=0)
    highest = jnp.max(stacked, axis=0)
    mixture = highest + jnp.log(jnp.sum(jnp.exp(stacked - highest[None]), axis=0))
    student_logits = jnp.dot(student_hidden, student_weight, preferred_element_type=jnp.float32)
    log_student = student_logits - log_total(student_logits)[:, None]
    divergence = jnp.sum(jnp.exp(mixture) * (mixture - log_student), axis=1)
    picked = jnp.take_along_axis(log_student, targets[:, None].astype(jnp.int32), axis=1)[:, 0]
    return divergence, -picked
```

```python
import jax
import jax.numpy as jnp
from jax import lax
from jax.experimental import pallas as pl
from jax.experimental.pallas import tpu as pltpu
from jax.sharding import PartitionSpec as P


SIDE = 4


def spot(x, y, core):
    return ((x % SIDE) * SIDE + y % SIDE) * 2 + core


def ring_turn(step, phase):
    pairs = []
    for x in range(SIDE):
        for y in range(SIDE):
            for core in range(2):
                along_x = core == phase
                there = spot(x + step, y, core) if along_x else spot(x, y + step, core)
                pairs.append((spot(x, y, core), there))
    return pairs


SWAP = [(v, v ^ 1) for v in range(2 * SIDE * SIDE)]
STEPS = (1, 3, 2)


def around(value, phase):
    return {k: lax.ppermute(value, "vocab", ring_turn(k, phase)) for k in STEPS}


def branch_send(value, step):
    return lax.ppermute(value, "branch", [(z, (z + step) % 4) for z in range(4)])


def slab_order():
    place = lax.axis_index("vocab")
    x, y, core = place // 8, (place // 2) % 4, place % 2
    order = []
    for second in (0, *STEPS):
        for mine in (True, False):
            side = core if mine else 1 - core
            for first in (0, *STEPS):
                x_first = spot(x - first, y - second, 0)
                y_first = spot(x - second, y - first, 1)
                order.append(jnp.where(side == 0, x_first, y_first))
    return jnp.stack(order).astype(jnp.int32)


def move_slab(order_ref, w_ref, out_ref):
    out_ref[...] = w_ref[...]


def reordered(weights, order):
    depth = weights.shape[0] // 32
    slabs = weights.reshape(32, depth, weights.shape[1])
    block = (1, depth, weights.shape[1])
    out = pl.pallas_call(
        move_slab,
        grid_spec=pltpu.PrefetchScalarGridSpec(
            num_scalar_prefetch=1,
            grid=(32,),
            in_specs=[pl.BlockSpec(block, lambda i, order: (order[i], 0, 0))],
            out_specs=pl.BlockSpec(block, lambda i, order: (i, 0, 0)),
        ),
        out_shape=jax.ShapeDtypeStruct(slabs.shape, slabs.dtype),
    )(order, slabs)
    return out.reshape(4, weights.shape[0] // 4, weights.shape[1])


def gathered_pieces(hidden):
    first = around(hidden, 0)
    strip = jnp.concatenate([hidden, *(first[k] for k in STEPS)], axis=1)
    second = around(strip, 1)
    pieces = []
    for piece in (strip, *(second[k] for k in STEPS)):
        pieces.append((piece, lax.ppermute(piece, "vocab", SWAP)))
    return pieces


def product(pieces, weights):
    total = None
    for k, (mine, other) in enumerate(pieces):
        part = jnp.dot(
            jnp.concatenate([mine, other], axis=1), weights[k], preferred_element_type=jnp.float32
        )
        total = part if total is None else total + part
    return total


def tell_all(value):
    copies = jnp.broadcast_to(value[None], (32, *value.shape))
    return lax.all_to_all(copies, "vocab", 0, 0, tiled=True)


def local_stats(logits):
    top = jnp.max(logits, axis=1)
    return top, jnp.sum(jnp.exp(logits - top[:, None]), axis=1)


def per_device(
    teacher_hidden,
    teacher_weight,
    student_hidden,
    student_weight,
    branch_weight,
    assignment,
    targets,
):
    order = slab_order()
    weights = reordered(teacher_weight[0], order)
    student_w = reordered(student_weight, order)
    width = student_weight.shape[1]
    rows = student_hidden.shape[0]
    group = lax.axis_index("branch")
    share = branch_weight / jnp.sum(branch_weight)
    log_share = jnp.log(share)[assignment]

    logits = product(gathered_pieces(teacher_hidden[0]), weights)
    top, total = local_stats(logits)
    relative, tops, totals = [], [], []
    for k in (0, 1, 3, 2):
        at = (group + k) % 4 * rows
        block_top = lax.dynamic_slice(top, (at,), (rows,))
        block = lax.dynamic_slice(logits, (at, 0), (rows, width)) - block_top[:, None]
        stats = jnp.stack([block_top, lax.dynamic_slice(total, (at,), (rows,))])
        if k:
            stats = branch_send(stats, k)
            block = branch_send(jnp.maximum(block, -60000.0).astype(jnp.float16), k)
        relative.append(block.astype(jnp.float32))
        tops.append(stats[0])
        totals.append(stats[1])
    tops, totals = jnp.stack(tops), jnp.stack(totals)
    sources = jnp.stack([(group - k) % 4 for k in (0, 1, 3, 2)])
    own_share = jnp.sum(
        jnp.where(sources[:, None] == jnp.arange(4)[None, :], log_share[None, :], 0.0), axis=1
    )
    everyone = tell_all(jnp.stack([tops, totals]))
    highest = jnp.max(everyone[:, 0], axis=0)
    summed = jnp.sum(everyone[:, 1] * jnp.exp(everyone[:, 0] - highest[None]), axis=0)
    offset = tops - highest - jnp.log(summed) + own_share[:, None]

    student_logits = product(gathered_pieces(student_hidden), student_w)
    student_top, student_total = local_stats(student_logits)
    columns = lax.axis_index("vocab") * width + jnp.arange(width, dtype=jnp.int32)
    matches = columns[None, :] == targets[:, None]
    picked = jnp.sum(jnp.where(matches, student_logits, 0.0), axis=1)

    mixture = sum(jnp.exp(block + offset[k][:, None]) for k, block in enumerate(relative))
    safe = jnp.where(mixture > 0.0, mixture, 1.0)
    against = jnp.log(safe) - (student_logits - student_top[:, None])
    part = jnp.sum(mixture * against, axis=1)
    mass = jnp.sum(mixture, axis=1)

    ends = tell_all(jnp.stack([part, mass, student_top, student_total, picked]))
    student_high = jnp.max(ends[:, 2], axis=0)
    student_sum = jnp.sum(ends[:, 3] * jnp.exp(ends[:, 2] - student_high[None]), axis=0)
    student_lse = student_high + jnp.log(student_sum)
    divergence = jnp.sum(ends[:, 0] + ends[:, 1] * (student_lse[None] - ends[:, 2]), axis=0)
    return divergence, student_lse - jnp.sum(ends[:, 4], axis=0)


def solution(mesh):
    in_specs = (
        P("branch", None, "vocab"),
        P("branch", None, "vocab"),
        P("branch", "vocab"),
        P(None, "vocab"),
        P(),
        P(),
        P("branch"),
    )
    out_specs = (P("branch"), P("branch"))
    return jax.shard_map(
        per_device, mesh=mesh, in_specs=in_specs, out_specs=out_specs, check_vma=False
    )
```

```python
import jax
import jax.numpy as jnp
from jax import lax
from jax.experimental import pallas as pl
from jax.experimental.pallas import tpu as pltpu
from jax.sharding import PartitionSpec as P


SIDE = 4
STEPS = (1, 3, 2)
SWAP = [(v, v ^ 1) for v in range(2 * SIDE * SIDE)]
BLOCKS = (0, 1, 3, 2)


def spot(x, y, core):
    return ((x % SIDE) * SIDE + y % SIDE) * 2 + core


def ring_turn(step, phase):
    pairs = []
    for x in range(SIDE):
        for y in range(SIDE):
            for core in range(2):
                along_x = core == phase
                there = spot(x + step, y, core) if along_x else spot(x, y + step, core)
                pairs.append((spot(x, y, core), there))
    return pairs


def branch_send(value, step):
    return lax.ppermute(value, "branch", [(z, (z + step) % 4) for z in range(4)])


def slab_order():
    place = lax.axis_index("vocab")
    x, y, core = place // 8, (place // 2) % 4, place % 2
    second, mine, first = (
        jnp.asarray(v, jnp.int32)
        for v in zip(*((s, m, f) for s in (0, *STEPS) for m in (1, 0) for f in (0, *STEPS)))
    )
    side = jnp.where(mine == 1, core, 1 - core)
    x_first = spot(x - first, y - second, 0)
    y_first = spot(x - second, y - first, 1)
    return jnp.where(side == 0, x_first, y_first).astype(jnp.int32)


def fetch(order_ref, w_ref, held, sems, first_slab, count):
    width = w_ref.shape[0]
    copies = []
    for i in range(count):
        at = pl.multiple_of(order_ref[first_slab + i] * 128, 128)
        copies.append(
            pltpu.make_async_copy(
                w_ref.at[:, pl.ds(at, 128)], held.at[pl.ds(0, width), pl.ds(i * 128, 128)], sems.at[i]
            )
        )
    for copy in copies:
        copy.start()
    return copies


def multiply(pieces, copies, held, total, fresh):
    per_piece = pieces[0].shape[1] // 128
    depth = pieces[0].shape[1]
    for g, piece in enumerate(pieces):
        for copy in copies[g * per_piece : (g + 1) * per_piece]:
            copy.wait()

        def columns(n, carry, g=g, piece=piece):
            at = pl.multiple_of(n * 256, 256)
            part = lax.dot_general(
                piece[...],
                held[pl.ds(at, 256), pl.ds(g * depth, depth)],
                (((1,), (1,)), ((), ())),
                preferred_element_type=jnp.float32,
            )
            if not (fresh and g == 0):
                part = part + total[:, pl.ds(at, 256)]
            total[:, pl.ds(at, 256)] = part
            return carry

        lax.fori_loop(0, 4, columns, 0)


def early_kernel(order_ref, *refs):
    *pieces, w_ref, total, held, sems = refs
    copies = fetch(order_ref, w_ref, held, sems, 0, held.shape[1] // 128)
    multiply(pieces, copies, held, total, True)


def late_kernel(order_ref, group_ref, *refs):
    *pieces, w_ref, before, b0, b1, b3, b2, top_ref, sum_ref, total, held, sems = refs
    copies = fetch(order_ref, w_ref, held, sems, 24, 8)
    width = w_ref.shape[0]
    total[...] = before[...]
    multiply(pieces, copies, held, total, False)
    rows = b0.shape[0]
    for j, (k, out) in enumerate(zip(BLOCKS, (b0, b1, b3, b2))):
        at = pl.multiple_of(lax.rem(group_ref[0] + k, 4) * rows, 64)
        block = total[pl.ds(at, rows), pl.ds(0, width)]
        top = jnp.max(block, axis=1, keepdims=True)
        block = block - top
        top_ref[pl.ds(j * rows, rows), :] = top
        sum_ref[pl.ds(j * rows, rows), :] = jnp.sum(jnp.exp(block), axis=1, keepdims=True)
        out[...] = jnp.maximum(block, -60000.0).astype(out.dtype)


def student_kernel(order_ref, *refs):
    *pieces, w_ref, out, top_ref, sum_ref, total, held, sems = refs
    copies = fetch(order_ref, w_ref, held, sems, 0, 32)
    multiply(pieces, copies, held, total, True)
    block = total[:, pl.ds(0, w_ref.shape[0])]
    top = jnp.max(block, axis=1, keepdims=True)
    block = block - top
    out[...] = block
    top_ref[...] = top
    sum_ref[...] = jnp.sum(jnp.exp(block), axis=1, keepdims=True)


VMEM = pl.BlockSpec(memory_space=pltpu.VMEM)
SMEM = pl.BlockSpec(memory_space=pltpu.SMEM)
HBM = pl.BlockSpec(memory_space=pl.ANY)
F32 = jnp.float32


def scratch(rows, depth):
    return [
        pltpu.VMEM((1024, depth), jnp.bfloat16),
        pltpu.SemaphoreType.DMA((depth // 128,)),
    ]


def teacher_early(order, pieces, w):
    rows = pieces[0].shape[0]
    return pl.pallas_call(
        early_kernel,
        in_specs=[SMEM] + [VMEM] * len(pieces) + [HBM],
        out_specs=VMEM,
        out_shape=jax.ShapeDtypeStruct((rows, 1024), F32),
        scratch_shapes=scratch(rows, 3072),
        name="teacher_early",
    )(order, *pieces, w)


def teacher_late(order, group, pieces, w, before, sent):
    rows, width = before.shape[0], w.shape[0]
    part = rows // 4
    return pl.pallas_call(
        late_kernel,
        in_specs=[SMEM, SMEM] + [VMEM] * len(pieces) + [HBM, VMEM],
        out_specs=[VMEM] * 6,
        out_shape=[jax.ShapeDtypeStruct((part, width), F32)]
        + [jax.ShapeDtypeStruct((part, width), sent)] * 3
        + [jax.ShapeDtypeStruct((rows, 1), F32)] * 2,
        scratch_shapes=[pltpu.VMEM((rows, 1024), F32)] + scratch(rows, 1024),
        name="teacher_late",
    )(order, group, *pieces, w, before)


def student_product(order, pieces, w):
    rows, width = pieces[0].shape[0], w.shape[0]
    return pl.pallas_call(
        student_kernel,
        in_specs=[SMEM] + [VMEM] * len(pieces) + [HBM],
        out_specs=[VMEM] * 3,
        out_shape=[jax.ShapeDtypeStruct((rows, width), F32)]
        + [jax.ShapeDtypeStruct((rows, 1), F32)] * 2,
        scratch_shapes=[pltpu.VMEM((rows, 1024), F32)] + scratch(rows, 4096),
        name="student_product",
    )(order, *pieces, w)


def around(value, phase):
    return {k: lax.ppermute(value, "vocab", ring_turn(k, phase)) for k in STEPS}


def first_phase(hidden):
    first = around(hidden, 0)
    return jnp.concatenate([hidden, *(first[k] for k in STEPS)], axis=1)


def second_phase(strip):
    second = around(strip, 1)
    return [strip, *(second[k] for k in STEPS)]


def paired(pieces):
    both = []
    for piece in pieces:
        both += [piece, lax.ppermute(piece, "vocab", SWAP)]
    return both


def tell_all(value):
    copies = jnp.broadcast_to(value[None], (32, *value.shape))
    return lax.all_to_all(copies, "vocab", 0, 0, tiled=True)


def per_device(
    teacher_hidden,
    teacher_weight,
    student_hidden,
    student_weight,
    branch_weight,
    assignment,
    targets,
):
    order = slab_order()
    w, student_w = teacher_weight[0].T, student_weight.T
    width, rows = w.shape[0], student_hidden.shape[0]
    group = lax.axis_index("branch")
    share = branch_weight / jnp.sum(branch_weight)
    log_share = jnp.log(share)[assignment]

    strip = first_phase(teacher_hidden[0])
    pieces = second_phase(strip)
    student_hidden, _ = lax.optimization_barrier((student_hidden, strip))
    student_strip = first_phase(student_hidden)

    pieces = paired(pieces)
    before = teacher_early(order, pieces[:6], w)
    student_strip, before = lax.optimization_barrier((student_strip, before))
    student_pieces = second_phase(student_strip)
    own, *sends, top, total = teacher_late(
        order, group[None].astype(jnp.int32), pieces[6:], w, before, SENT
    )
    stats = jnp.stack([top.reshape(4, rows), total.reshape(4, rows)], axis=1)
    relative, got = [own], [stats[0]]
    for j, k in enumerate(BLOCKS):
        if k:
            got.append(branch_send(stats[j], k))
    for j, k in enumerate(BLOCKS):
        if k:
            relative.append(branch_send(sends[j - 1].astype(jnp.float16), k).astype(F32))
    got = jnp.stack(got)
    sources = jnp.stack([(group - k) % 4 for k in BLOCKS])
    own_share = jnp.sum(
        jnp.where(sources[:, None] == jnp.arange(4)[None, :], log_share[None, :], 0.0), axis=1
    )
    everyone = tell_all(got)
    highest = jnp.max(everyone[:, :, 0], axis=0)
    summed = jnp.sum(everyone[:, :, 1] * jnp.exp(everyone[:, :, 0] - highest[None]), axis=0)
    offset = got[:, 0] - highest - jnp.log(summed) + own_share[:, None]

    student, student_top, student_total = student_product(order, paired(student_pieces), student_w)
    student_top, student_total = student_top[:, 0], student_total[:, 0]
    columns = lax.axis_index("vocab") * width + jnp.arange(width, dtype=jnp.int32)
    matches = columns[None, :] == targets[:, None]
    picked = jnp.sum(jnp.where(matches, student + student_top[:, None], 0.0), axis=1)

    mixture = sum(jnp.exp(block + offset[j][:, None]) for j, block in enumerate(relative))
    safe = jnp.where(mixture > 0.0, mixture, 1.0)
    part = jnp.sum(mixture * (jnp.log(safe) - student), axis=1)
    mass = jnp.sum(mixture, axis=1)

    ends = tell_all(jnp.stack([part, mass, student_top, student_total, picked]))
    student_high = jnp.max(ends[:, 2], axis=0)
    student_sum = jnp.sum(ends[:, 3] * jnp.exp(ends[:, 2] - student_high[None]), axis=0)
    student_lse = student_high + jnp.log(student_sum)
    divergence = jnp.sum(ends[:, 0] + ends[:, 1] * (student_lse[None] - ends[:, 2]), axis=0)
    return divergence, student_lse - jnp.sum(ends[:, 4], axis=0)


SENT = F32


def solution(mesh):
    in_specs = (
        P("branch", None, "vocab"),
        P("branch", None, "vocab"),
        P("branch", "vocab"),
        P(None, "vocab"),
        P(),
        P(),
        P("branch"),
    )
    out_specs = (P("branch"), P("branch"))
    return jax.shard_map(
        per_device, mesh=mesh, in_specs=in_specs, out_specs=out_specs, check_vma=False
    )
```
